32 devices in a mesh: section: 2 (over y), pen: 8 (over z, x), slab: 2 (over core).
Axes of the slice: x: 2, y: 2, z: 4, core: 2. Of those that a mesh axis runs over, the one named last changes fastest.
Arguments:
- velocity: float32 [3, 48, 48, 48], P(None, ('section', 'pen'), 'slab'), may hold values from -6 to 6
- vorticity: float32 [3, 48, 48, 48], P(None, ('section', 'pen'), 'slab'), may hold values from -6 to 6
- velocity_modes: float32 [3, 32, 32, 2, 32], P(None, None, ('section', 'pen'), None, 'slab'), may hold values from -6 to 6
Outputs:
- rhs_modes: float32 [3, 32, 32, 2, 32], P(None, None, ('section', 'pen'), None, 'slab')
The draws below stay inside these ranges and needn't reach their ends.
All inputs are finite; a program needn't handle non-finite values.
Results may differ from the reference program's by a relative error of at most 0.000057.
Values sent between devices are 32-bit elements; how exact they have to be, the bound alone decides.
A program may use at most 64 MiB of HBM per device.

```python
import jax
import jax.numpy as jnp
from jax import lax

N = 48
KEEP = 32


def block_levels(stream_key, shape, split, low, top_value):
    def one(position, blocks):
        steps = jax.random.uniform(jax.random.fold_in(jax.random.fold_in(stream_key, 6), position), (blocks,), jnp.float32, low / len(split), top_value / len(split))
        return jnp.repeat(jnp.exp(steps), shape[position] // blocks).reshape((-1,) + (1,) * (len(shape) - position - 1))

    loudness = one(*split[0])
    for cut in split[1:]:
        loudness = loudness * one(*cut)
    return loudness


def centred(stream_key, shape, deviation, most, split=(), kind=jnp.bfloat16):
    drawn = deviation * jax.random.normal(stream_key, shape, jnp.float32)
    if split:
        drawn = drawn * block_levels(stream_key, shape, split, -0.22, 0.18)
    return jnp.clip(drawn, -most, most).astype(kind)


def setup_inputs(seed: int = 0) -> dict:
    streams_of = jax.random.split(jax.random.key(seed), 4)
    return {
        "velocity": centred(streams_of[0], (3, N, N, N), 1.0, 6.0, ((1, 16), (2, 2)), jnp.float32),
        "vorticity": centred(streams_of[1], (3, N, N, N), 1.0, 6.0, ((1, 16), (2, 2)), jnp.float32),
        "velocity_modes": centred(streams_of[2], (3, KEEP, KEEP, 2, KEEP), 1.0, 6.0, ((2, 16), (4, 2)), jnp.float32),
    }


def signed_modes(index, count):
    return jnp.where(index < count // 2, index, index - count)


def reference(velocity, vorticity, velocity_modes):
    velocity_field = velocity
    vorticity_field = vorticity
    cross_product = jnp.stack([velocity_field[1] * vorticity_field[2] - velocity_field[2] * vorticity_field[1],
                         velocity_field[2] * vorticity_field[0] - velocity_field[0] * vorticity_field[2],
                         velocity_field[0] * vorticity_field[1] - velocity_field[1] * vorticity_field[0]])
    picked = jnp.concatenate([jnp.arange(KEEP // 2, dtype=jnp.int32),
                              jnp.arange(N - KEEP // 2, N, dtype=jnp.int32)])

    def transform(field):
        spec = jnp.fft.fft(field, axis=2, norm="ortho")[:, :, picked]
        spec = jnp.fft.fft(spec, axis=1, norm="ortho")[:, picked, :]
        spec = jnp.fft.fft(spec, axis=0, norm="ortho")[picked]
        return jnp.stack([jnp.real(spec), jnp.imag(spec)])

    spectrum = lax.map(transform, cross_product)
    modes = signed_modes(jnp.arange(KEEP, dtype=jnp.int32), KEEP)
    kz = modes[:, None, None]
    ky = modes[None, :, None]
    kx = modes[None, None, :]
    limit = -(KEEP // 2)
    mask = ((kx != limit) & (ky != limit) & (kz != limit)).astype(jnp.float32)
    waves = (kx.astype(jnp.float32), ky.astype(jnp.float32), kz.astype(jnp.float32))
    ksq = waves[0] * waves[0] + waves[1] * waves[1] + waves[2] * waves[2]
    denom = jnp.maximum(ksq, 1.0)
    parts = []
    for which in range(2):
        comp = [spectrum[c, which] for c in range(3)]
        inner = (waves[0] * comp[0] + waves[1] * comp[1] + waves[2] * comp[2]) / denom
        parts.append(jnp.stack([comp[c] - waves[c] * inner for c in range(3)]))
    projected = jnp.stack(parts, axis=3)
    visc = 0.5 / (KEEP // 2) ** 2
    return projected * mask[None, :, :, None, :] - visc * ksq[None, :, :, None, :] * velocity_modes
```

```python
import functools
import math

import jax
import jax.numpy as jnp
import numpy as np
from jax import lax
from jax.experimental import pallas as pl
from jax.experimental.pallas import tpu as pltpu
from jax.sharding import PartitionSpec as P

AXES = ("section", "pen", "slab")
highest = lax.Precision.HIGHEST


def signed_modes(index, count):
    return jnp.where(index < count // 2, index, index - count)


def discrete_fourier_tables(length, keep_count):
    modes = signed_modes(jnp.arange(keep_count, dtype=jnp.int32), keep_count)
    mode_positions = jnp.arange(length, dtype=jnp.int32)
    phase = jnp.remainder(modes[:, None] * mode_positions[None, :], length).astype(jnp.float32)
    angles = 2.0 * math.pi / length * phase
    factor = 1.0 / math.sqrt(length)
    return (jnp.cos(angles) * factor, jnp.sin(angles) * factor)


def complex_apply(form, cosine, sine, real_part, imag_part):
    out_real = jnp.einsum(form, cosine, real_part, precision=highest) + jnp.einsum(
        form, sine, imag_part, precision=highest
    )
    out_imag = jnp.einsum(form, cosine, imag_part, precision=highest) - jnp.einsum(
        form, sine, real_part, precision=highest
    )
    return (out_real, out_imag)


def per_device(velocity, vorticity, velocity_modes):
    grid_cells = velocity.shape[3]
    keep_count = velocity_modes.shape[1]
    cross_product = jnp.stack(
        [
            velocity[1] * vorticity[2] - velocity[2] * vorticity[1],
            velocity[2] * vorticity[0] - velocity[0] * vorticity[2],
            velocity[0] * vorticity[1] - velocity[1] * vorticity[0],
        ]
    )
    slabs = lax.axis_size("slab")
    block_modes = keep_count // slabs
    cosine_table, sine_table = discrete_fourier_tables(grid_cells, keep_count)
    cols_real = cosine_table.T.reshape(grid_cells, slabs, block_modes)
    cols_imag = (-sine_table).T.reshape(grid_cells, slabs, block_modes)
    column_table = jnp.stack([cols_real, cols_imag], axis=2).reshape(grid_cells, 2 * keep_count)
    first_pass = jnp.einsum("czyx,xj->czyj", cross_product, column_table, precision=highest)
    block = lax.all_to_all(first_pass, "slab", split_axis=3, concat_axis=2, tiled=True)
    out_real, out_imag = complex_apply(
        "ky,czyj->czkj",
        cosine_table,
        sine_table,
        block[..., :block_modes],
        block[..., block_modes:],
    )
    second_pass = jnp.concatenate([out_real, out_imag], axis=-1)
    halves = lax.axis_size("section")
    pens = lax.axis_size("pen")
    rows_ky = keep_count // (halves * pens)
    block = lax.all_to_all(second_pass, ("section", "pen"), split_axis=2, concat_axis=1, tiled=True)
    out_real, out_imag = complex_apply(
        "kz,czyj->ckyj",
        cosine_table,
        sine_table,
        block[..., :block_modes],
        block[..., block_modes:],
    )
    third_pass = jnp.concatenate([out_real, out_imag], axis=-1)
    group_index = lax.axis_index("section") * pens + lax.axis_index("pen")
    modes_z = signed_modes(jnp.arange(keep_count, dtype=jnp.int32), keep_count)[:, None, None]
    modes_y = signed_modes(
        group_index * rows_ky + jnp.arange(rows_ky, dtype=jnp.int32), keep_count
    )[None, :, None]
    modes_x = signed_modes(
        lax.axis_index("slab") * block_modes + jnp.arange(block_modes, dtype=jnp.int32), keep_count
    )[None, None, :]
    limit = -(keep_count // 2)
    keep_mask = ((modes_x != limit) & (modes_y != limit) & (modes_z != limit)).astype(jnp.float32)
    waves = (modes_x.astype(jnp.float32), modes_y.astype(jnp.float32), modes_z.astype(jnp.float32))
    ksq = waves[0] * waves[0] + waves[1] * waves[1] + waves[2] * waves[2]
    denom = jnp.maximum(ksq, 1.0)
    parts = []
    for which in range(2):
        chosen = third_pass[..., which * block_modes : (which + 1) * block_modes]
        comp = [chosen[c] for c in range(3)]
        inner = (waves[0] * comp[0] + waves[1] * comp[1] + waves[2] * comp[2]) / denom
        parts.append(jnp.stack([comp[c] - waves[c] * inner for c in range(3)]))
    projected = jnp.stack(parts, axis=3)
    visc = 0.5 / (keep_count // 2) ** 2
    return (
        projected * keep_mask[None, :, :, None, :]
        - visc * ksq[None, :, :, None, :] * velocity_modes
    )


def split_bf16(table):
    high = table.astype(jnp.bfloat16)
    low = (table - high.astype(np.float32)).astype(jnp.bfloat16)
    return high, low


def split_in_kernel(value):
    high = value.astype(jnp.bfloat16)
    low = (value - high.astype(jnp.float32)).astype(jnp.bfloat16)
    return high, low


def mm(a, b):
    return lax.dot_general(a, b, (((1,), (0,)), ((), ())), preferred_element_type=jnp.float32)


def split_dot(a, b):
    return mm(a[0], b[0]) + mm(a[1], b[0]) + mm(a[0], b[1])


def wave_numbers(count):
    index = np.arange(count)
    return np.where(index < count // 2, index, index - count)


def host_tables(cells, keep):
    phase = np.remainder(wave_numbers(keep)[:, None] * np.arange(cells)[None, :], cells)
    angles = 2.0 * np.pi / cells * phase
    factor = 1.0 / np.sqrt(cells)
    return np.cos(angles) * factor, np.sin(angles) * factor


class Plan:
    def __init__(self, mesh_shape, cells, keep, z_rows, y_rows):
        self.cells, self.keep, self.z_rows, self.y_rows = cells, keep, z_rows, y_rows
        self.halves, self.pens, self.slabs = (mesh_shape[a] for a in AXES)
        self.groups = self.halves * self.pens
        self.count = self.groups * self.slabs
        self.rows_ky = keep // self.groups
        self.block = keep // self.slabs
        self.field = self.rows_ky * 2 * self.block
        self.rows = z_rows + (z_rows + 1) // 2
        self.slots = 2 * self.rows_ky

    def fits(self):
        return (
            2 * self.field == 128
            and self.rows <= 8
            and (self.rows * self.groups) % 16 == 0
            and self.y_rows % 8 == 0
            and self.keep % 8 == 0
            and self.block % 8 == 0
            and 3 * self.z_rows * self.y_rows <= 512
            and self.count <= 64
        )

    def place(self, comp, z):
        if comp < 2:
            return z, comp
        return self.z_rows + z // 2, z % 2

    def tables(self):
        cos, sin = host_tables(self.cells, self.keep)
        g, zl, yl, ky_n, bm = self.groups, self.z_rows, self.y_rows, self.rows_ky, self.block
        first = np.zeros((self.slabs, self.slots, 2, self.rows, g, 3, zl, yl), np.float32)
        for c in range(3):
            for z in range(zl):
                row, half = self.place(c, z)
                for ky in range(ky_n):
                    for s in range(self.slabs):
                        cells = slice(s * yl, (s + 1) * yl)
                        first[s, half * ky_n + ky, 0, row, :, c, z] = cos[ky::ky_n, cells]
                        first[s, half * ky_n + ky, 1, row, :, c, z] = -sin[ky::ky_n, cells]
        first = first.reshape(self.slabs, self.slots * 2 * self.rows * g, 3 * zl * yl)
        second = np.zeros((self.slots, 2, self.cells, self.slabs, self.slots, 2, bm), np.float32)
        for s in range(self.slabs):
            c_t = cos[s * bm : (s + 1) * bm].T
            s_t = sin[s * bm : (s + 1) * bm].T
            for q in range(self.slots):
                second[q, 0, :, s, q, 0] = c_t
                second[q, 0, :, s, q, 1] = -s_t
                second[q, 1, :, s, q, 0] = s_t
                second[q, 1, :, s, q, 1] = c_t
        second = second.reshape(self.slots * 2, self.cells, self.slabs * 128)
        third = np.zeros((3, 2, self.keep, g, self.slabs, 8), np.float32)
        for z in range(zl):
            for which, table in enumerate((cos, sin)):
                column = table[:, z::zl][:, :, None]
                third[0, which, :, :, :, z] = column
                third[1 + z % 2, which, :, :, :, zl + z // 2] = column
        third = third.reshape(6 * self.keep, self.count * 8)
        return (
            np.stack(split_bf16(first), axis=1),
            np.stack(split_bf16(second)),
            np.stack(split_bf16(third)),
        )


def kernel(
    plan, vel_hbm, vort_hbm, modes_hbm, first_hbm, second_hbm, third_hbm, out_ref,
    vel, vort, modes, first, second, third, send, recv, load_sem, send_sem, recv_sem,
):
    sec, pen, slab = (lax.axis_index(a) for a in AXES)
    group = sec * plan.pens + pen
    me = group * plan.slabs + slab
    loads = [
        pltpu.make_async_copy(src, dst, load_sem.at[i])
        for i, (src, dst) in enumerate(
            (
                (vel_hbm, vel),
                (vort_hbm, vort),
                (first_hbm.at[slab], first),
                (second_hbm, second),
                (third_hbm, third),
                (modes_hbm, modes),
            )
        )
    ]
    for load in loads:
        load.start()

    def spread(offset):
        a, b, c = offset
        to = (
            lax.rem(sec + a, plan.halves),
            lax.rem(pen + b, plan.pens),
            lax.rem(slab + c, plan.slabs),
        )
        back = (
            lax.rem(sec + plan.halves - a, plan.halves),
            lax.rem(pen + plan.pens - b, plan.pens),
            lax.rem(slab + plan.slabs - c, plan.slabs),
        )
        return to, (back[0] * plan.pens + back[1]) * plan.slabs + back[2]

    offsets = [
        (a, b, c)
        for b in sorted(range(plan.pens), key=lambda v: -min(v, plan.pens - v))
        for a in reversed(range(plan.halves))
        for c in reversed(range(plan.slabs))
    ]
    offsets.remove((0, 0, 0))
    recv[...] = jnp.zeros_like(recv)
    barrier = pltpu.get_barrier_semaphore()
    for offset in offsets:
        pl.semaphore_signal(
            barrier, inc=1, device_id=spread(offset)[0], device_id_type=pl.DeviceIdType.MESH
        )

    loads[0].wait()
    loads[1].wait()
    zl, yl, cells = plan.z_rows, plan.y_rows, plan.cells
    v = [vel[c].reshape(zl * yl, cells) for c in range(3)]
    w = [vort[c].reshape(zl * yl, cells) for c in range(3)]
    cross = jnp.concatenate(
        [v[1] * w[2] - v[2] * w[1], v[2] * w[0] - v[0] * w[2], v[0] * w[1] - v[1] * w[0]], axis=0
    )
    cross = split_in_kernel(cross)
    loads[2].wait()
    part = split_dot((first[0], first[1]), cross)
    part = split_in_kernel(part)
    loads[3].wait()
    size = plan.rows * plan.groups
    total = None
    for i in range(2 * plan.slots):
        piece = tuple(p[i * size : (i + 1) * size] for p in part)
        term = split_dot(piece, (second[0, i], second[1, i]))
        total = term if total is None else total + term
    for s in range(plan.slabs):
        for r in range(plan.rows):
            send[s, :, r, :] = total[r * plan.groups : (r + 1) * plan.groups, s * 128 : (s + 1) * 128]

    pl.semaphore_wait(barrier, plan.count - 1)
    used = pl.ds(0, plan.rows)
    copies = []
    for i, offset in enumerate(offsets):
        to, source = spread(offset)
        copy = pltpu.make_async_remote_copy(
            src_ref=send.at[to[2], to[0] * plan.pens + to[1], used],
            dst_ref=recv.at[me, used],
            send_sem=send_sem.at[i],
            recv_sem=recv_sem.at[i],
            device_id=to,
            device_id_type=pl.DeviceIdType.MESH,
        )
        copy.start()
        arrival = pltpu.make_async_remote_copy(
            src_ref=send.at[to[2], to[0] * plan.pens + to[1], used],
            dst_ref=recv.at[source, used],
            send_sem=send_sem.at[i],
            recv_sem=recv_sem.at[i],
            device_id=to,
            device_id_type=pl.DeviceIdType.MESH,
        )
        copies.append((copy, arrival))
    recv[me, 0 : plan.rows] = send[slab, group, 0 : plan.rows]

    keep, bm, ky_n = plan.keep, plan.block, plan.rows_ky

    def signed(index):
        return jnp.where(index < keep // 2, index, index - keep)

    lane = lax.broadcasted_iota(jnp.int32, (keep, 128), 1)
    inner_lane = lax.rem(lane, plan.field)
    low_half = lane < plan.field
    is_real = lax.rem(lane // bm, 2) == 0
    kx = signed(lax.rem(lane, bm) + slab * bm)
    ky = signed(inner_lane // (2 * bm) + group * ky_n)
    kz = signed(lax.broadcasted_iota(jnp.int32, (keep, 128), 0))
    limit = -(keep // 2)
    mask = ((kx != limit) & (ky != limit) & (kz != limit)).astype(jnp.float32)
    kx, ky, kz = (k.astype(jnp.float32) for k in (kx, ky, kz))
    inverse = 1.0 / jnp.maximum(kx * kx + ky * ky + kz * kz, 1.0)
    pair = jnp.where(low_half, kx, ky)

    row = lax.broadcasted_iota(jnp.int32, (plan.field, keep), 0)
    kz_t = signed(lax.broadcasted_iota(jnp.int32, (plan.field, keep), 1)).astype(jnp.float32)
    kx_t = signed(lax.rem(row, bm) + slab * bm).astype(jnp.float32)
    ky_t = signed(row // (2 * bm) + group * ky_n).astype(jnp.float32)
    visc = 0.5 / (keep // 2) ** 2
    damp = visc * (kx_t * kx_t + ky_t * ky_t + kz_t * kz_t)
    loads[5].wait()
    damped = [damp * modes[c].reshape(plan.field, keep) for c in range(3)]
    loads[4].wait()

    for _, arrival in copies:
        arrival.wait_recv()
    got = split_in_kernel(recv[...].reshape(plan.count * 8, 128))
    out = split_dot((third[0], third[1]), got)
    out = [out[i * keep : (i + 1) * keep] for i in range(6)]

    def turn(cos_part, sin_part):
        ahead = pltpu.roll(sin_part, 128 - bm, 1)
        behind = pltpu.roll(sin_part, bm, 1)
        return cos_part + jnp.where(is_real, ahead, -behind)

    both = turn(out[0], out[1])
    last_cos = jnp.where(low_half, out[2], out[4])
    last_sin = jnp.where(low_half, out[3], out[5])
    last = turn(last_cos, last_sin)
    last = last + pltpu.roll(last, plan.field, 1)
    dots = pair * both
    inner = (dots + pltpu.roll(dots, plan.field, 1) + kz * last) * inverse
    both = jnp.transpose((both - pair * inner) * mask)
    last = jnp.transpose((last - kz * inner) * mask)
    shape = (ky_n, 2, bm, keep)
    out_ref[0] = (both[: plan.field] - damped[0]).reshape(shape)
    out_ref[1] = (both[plan.field :] - damped[1]).reshape(shape)
    out_ref[2] = (last[: plan.field] - damped[2]).reshape(shape)
    for copy, _ in copies:
        copy.wait_send()


def direct(plan, tables, velocity, vorticity, velocity_modes):
    modes = jnp.transpose(velocity_modes, (0, 2, 3, 4, 1))
    first, second, third = tables
    hbm = pl.BlockSpec(memory_space=pl.ANY)
    out = pl.pallas_call(
        functools.partial(kernel, plan),
        out_shape=jax.ShapeDtypeStruct(modes.shape, jnp.float32),
        in_specs=[hbm] * 6,
        out_specs=pl.BlockSpec(memory_space=pltpu.VMEM),
        scratch_shapes=[
            pltpu.VMEM(velocity.shape, jnp.float32),
            pltpu.VMEM(vorticity.shape, jnp.float32),
            pltpu.VMEM(modes.shape, jnp.float32),
            pltpu.VMEM(first.shape[1:], jnp.bfloat16),
            pltpu.VMEM(second.shape, jnp.bfloat16),
            pltpu.VMEM(third.shape, jnp.bfloat16),
            pltpu.VMEM((plan.slabs, plan.groups, 8, 128), jnp.float32),
            pltpu.VMEM((plan.count, 8, 128), jnp.float32),
            pltpu.SemaphoreType.DMA((6,)),
            pltpu.SemaphoreType.DMA((plan.count - 1,)),
            pltpu.SemaphoreType.DMA((plan.count - 1,)),
        ],
        compiler_params=pltpu.CompilerParams(collective_id=0, has_side_effects=True),
    )(velocity, vorticity, modes, first, second, third)
    return jnp.transpose(out, (0, 4, 1, 2, 3))


def solution(mesh):
    sizes = dict(mesh.shape)

    def run(velocity, vorticity, velocity_modes):
        _, z_rows, y_rows, cells = velocity.shape
        plan = Plan(sizes, cells, velocity_modes.shape[1], z_rows, y_rows)
        if not plan.fits():
            return per_device(velocity, vorticity, velocity_modes)
        return direct(plan, plan.tables(), velocity, vorticity, velocity_modes)

    return jax.shard_map(
        run,
        mesh=mesh,
        in_specs=(
            P(None, ("section", "pen"), "slab", None),
            P(None, ("section", "pen"), "slab", None),
            P(None, None, ("section", "pen"), None, "slab"),
        ),
        out_specs=P(None, None, ("section", "pen"), None, "slab"),
        check_vma=False,
    )
```

```python
import functools
import math

import jax
import jax.numpy as jnp
import numpy as np
from jax import lax
from jax.experimental import pallas as pl
from jax.experimental.pallas import tpu as pltpu
from jax.sharding import PartitionSpec as P

AXES = ("section", "pen", "slab")
highest = lax.Precision.HIGHEST


def signed_modes(index, count):
    return jnp.where(index < count // 2, index, index - count)


def discrete_fourier_tables(length, keep_count):
    modes = signed_modes(jnp.arange(keep_count, dtype=jnp.int32), keep_count)
    mode_positions = jnp.arange(length, dtype=jnp.int32)
    phase = jnp.remainder(modes[:, None] * mode_positions[None, :], length).astype(jnp.float32)
    angles = 2.0 * math.pi / length * phase
    factor = 1.0 / math.sqrt(length)
    return (jnp.cos(angles) * factor, jnp.sin(angles) * factor)


def complex_apply(form, cosine, sine, real_part, imag_part):
    out_real = jnp.einsum(form, cosine, real_part, precision=highest) + jnp.einsum(
        form, sine, imag_part, precision=highest
    )
    out_imag = jnp.einsum(form, cosine, imag_part, precision=highest) - jnp.einsum(
        form, sine, real_part, precision=highest
    )
    return (out_real, out_imag)


def per_device(velocity, vorticity, velocity_modes):
    grid_cells = velocity.shape[3]
    keep_count = velocity_modes.shape[1]
    cross_product = jnp.stack(
        [
            velocity[1] * vorticity[2] - velocity[2] * vorticity[1],
            velocity[2] * vorticity[0] - velocity[0] * vorticity[2],
            velocity[0] * vorticity[1] - velocity[1] * vorticity[0],
        ]
    )
    slabs = lax.axis_size("slab")
    block_modes = keep_count // slabs
    cosine_table, sine_table = discrete_fourier_tables(grid_cells, keep_count)
    cols_real = cosine_table.T.reshape(grid_cells, slabs, block_modes)
    cols_imag = (-sine_table).T.reshape(grid_cells, slabs, block_modes)
    column_table = jnp.stack([cols_real, cols_imag], axis=2).reshape(grid_cells, 2 * keep_count)
    first_pass = jnp.einsum("czyx,xj->czyj", cross_product, column_table, precision=highest)
    block = lax.all_to_all(first_pass, "slab", split_axis=3, concat_axis=2, tiled=True)
    out_real, out_imag = complex_apply(
        "ky,czyj->czkj",
        cosine_table,
        sine_table,
        block[..., :block_modes],
        block[..., block_modes:],
    )
    second_pass = jnp.concatenate([out_real, out_imag], axis=-1)
    halves = lax.axis_size("section")
    pens = lax.axis_size("pen")
    rows_ky = keep_count // (halves * pens)
    block = lax.all_to_all(second_pass, ("section", "pen"), split_axis=2, concat_axis=1, tiled=True)
    out_real, out_imag = complex_apply(
        "kz,czyj->ckyj",
        cosine_table,
        sine_table,
        block[..., :block_modes],
        block[..., block_modes:],
    )
    third_pass = jnp.concatenate([out_real, out_imag], axis=-1)
    group_index = lax.axis_index("section") * pens + lax.axis_index("pen")
    modes_z = signed_modes(jnp.arange(keep_count, dtype=jnp.int32), keep_count)[:, None, None]
    modes_y = signed_modes(
        group_index * rows_ky + jnp.arange(rows_ky, dtype=jnp.int32), keep_count
    )[None, :, None]
    modes_x = signed_modes(
        lax.axis_index("slab") * block_modes + jnp.arange(block_modes, dtype=jnp.int32), keep_count
    )[None, None, :]
    limit = -(keep_count // 2)
    keep_mask = ((modes_x != limit) & (modes_y != limit) & (modes_z != limit)).astype(jnp.float32)
    waves = (modes_x.astype(jnp.float32), modes_y.astype(jnp.float32), modes_z.astype(jnp.float32))
    ksq = waves[0] * waves[0] + waves[1] * waves[1] + waves[2] * waves[2]
    denom = jnp.maximum(ksq, 1.0)
    parts = []
    for which in range(2):
        chosen = third_pass[..., which * block_modes : (which + 1) * block_modes]
        comp = [chosen[c] for c in range(3)]
        inner = (waves[0] * comp[0] + waves[1] * comp[1] + waves[2] * comp[2]) / denom
        parts.append(jnp.stack([comp[c] - waves[c] * inner for c in range(3)]))
    projected = jnp.stack(parts, axis=3)
    visc = 0.5 / (keep_count // 2) ** 2
    return (
        projected * keep_mask[None, :, :, None, :]
        - visc * ksq[None, :, :, None, :] * velocity_modes
    )


def split_bf16(table):
    high = table.astype(jnp.bfloat16)
    low = (table - high.astype(np.float32)).astype(jnp.bfloat16)
    return high, low


def split_in_kernel(value):
    high = value.astype(jnp.bfloat16)
    low = (value - high.astype(jnp.float32)).astype(jnp.bfloat16)
    return high, low


def mm(a, b):
    return lax.dot_general(a, b, (((1,), (0,)), ((), ())), preferred_element_type=jnp.float32)


def split_dot(a, b):
    return mm(a[0], b[0]) + mm(a[1], b[0]) + mm(a[0], b[1])


def wave_numbers(count):
    index = np.arange(count)
    return np.where(index < count // 2, index, index - count)


def host_tables(cells, keep):
    phase = np.remainder(wave_numbers(keep)[:, None] * np.arange(cells)[None, :], cells)
    angles = 2.0 * np.pi / cells * phase
    factor = 1.0 / np.sqrt(cells)
    return np.cos(angles) * factor, np.sin(angles) * factor


class Plan:
    def __init__(self, mesh_shape, cells, keep, z_rows, y_rows):
        self.cells, self.keep, self.z_rows, self.y_rows = cells, keep, z_rows, y_rows
        self.halves, self.pens, self.slabs = (mesh_shape[a] for a in AXES)
        self.groups = self.halves * self.pens
        self.count = self.groups * self.slabs
        self.rows_ky = keep // self.groups
        self.block = keep // self.slabs
        self.field = self.rows_ky * 2 * self.block
        self.rows = z_rows + (z_rows + 1) // 2
        self.slots = 2 * self.rows_ky

    def fits(self):
        return (
            2 * self.field == 128
            and self.rows <= 8
            and (self.rows * self.groups) % 16 == 0
            and self.y_rows % 8 == 0
            and self.keep % 8 == 0
            and self.block % 8 == 0
            and 3 * self.z_rows * self.y_rows <= 512
            and self.count <= 64
        )

    def place(self, comp, z):
        if comp < 2:
            return z, comp
        return self.z_rows + z // 2, z % 2

    def tables(self):
        cos, sin = host_tables(self.cells, self.keep)
        g, zl, yl, ky_n, bm = self.groups, self.z_rows, self.y_rows, self.rows_ky, self.block
        first = np.zeros((self.slabs, self.slots, 2, self.rows, g, 3, zl, yl), np.float32)
        for c in range(3):
            for z in range(zl):
                row, half = self.place(c, z)
                for ky in range(ky_n):
                    for s in range(self.slabs):
                        cells = slice(s * yl, (s + 1) * yl)
                        first[s, half * ky_n + ky, 0, row, :, c, z] = cos[ky::ky_n, cells]
                        first[s, half * ky_n + ky, 1, row, :, c, z] = -sin[ky::ky_n, cells]
        first = first.reshape(self.slabs, self.slots * 2 * self.rows * g, 3 * zl * yl)
        second = np.zeros((self.slots, 2, self.cells, self.slabs, self.slots, 2, bm), np.float32)
        for s in range(self.slabs):
            c_t = cos[s * bm : (s + 1) * bm].T
            s_t = sin[s * bm : (s + 1) * bm].T
            for q in range(self.slots):
                second[q, 0, :, s, q, 0] = c_t
                second[q, 0, :, s, q, 1] = -s_t
                second[q, 1, :, s, q, 0] = s_t
                second[q, 1, :, s, q, 1] = c_t
        second = second.reshape(self.slots * 2, self.cells, self.slabs * 128)
        third = np.zeros((3, 2, self.keep, g, self.slabs, 8), np.float32)
        for z in range(zl):
            for which, table in enumerate((cos, sin)):
                column = table[:, z::zl][:, :, None]
                third[0, which, :, :, :, z] = column
                third[1 + z % 2, which, :, :, :, zl + z // 2] = column
        third = third.reshape(6 * self.keep, self.count * 8)
        return (
            np.stack(split_bf16(first), axis=1),
            np.stack(split_bf16(second)),
            np.stack(split_bf16(third)),
        )


def kernel(
    plan, vel_hbm, vort_hbm, modes_hbm, first_hbm, second_hbm, third_hbm, out_ref,
    vel, vort, modes, first, second, third, send, recv, load_sem, send_sem, recv_sem,
):
    sec, pen, slab = (lax.axis_index(a) for a in AXES)
    group = sec * plan.pens + pen
    me = group * plan.slabs + slab
    loads = [
        pltpu.make_async_copy(src, dst, load_sem.at[i])
        for i, (src, dst) in enumerate(
            (
                (vel_hbm, vel),
                (vort_hbm, vort),
                (first_hbm.at[slab], first),
                (second_hbm, second),
                (third_hbm, third),
                (modes_hbm, modes),
            )
        )
    ]
    for load in loads:
        load.start()

    def spread(offset):
        a, b, c = offset
        to = (
            lax.rem(sec + a, plan.halves),
            lax.rem(pen + b, plan.pens),
            lax.rem(slab + c, plan.slabs),
        )
        back = (
            lax.rem(sec + plan.halves - a, plan.halves),
            lax.rem(pen + plan.pens - b, plan.pens),
            lax.rem(slab + plan.slabs - c, plan.slabs),
        )
        return to, (back[0] * plan.pens + back[1]) * plan.slabs + back[2]

    offsets = [
        (a, b, c)
        for b in sorted(range(plan.pens), key=lambda v: -min(v, plan.pens - v))
        for a in reversed(range(plan.halves))
        for c in reversed(range(plan.slabs))
    ]
    offsets.remove((0, 0, 0))
    recv[...] = jnp.zeros_like(recv)
    barrier = pltpu.get_barrier_semaphore()
    for offset in offsets:
        pl.semaphore_signal(
            barrier, inc=1, device_id=spread(offset)[0], device_id_type=pl.DeviceIdType.MESH
        )

    loads[0].wait()
    loads[1].wait()
    zl, yl, cells = plan.z_rows, plan.y_rows, plan.cells
    v = [vel[c].reshape(zl * yl, cells) for c in range(3)]
    w = [vort[c].reshape(zl * yl, cells) for c in range(3)]
    cross = jnp.concatenate(
        [v[1] * w[2] - v[2] * w[1], v[2] * w[0] - v[0] * w[2], v[0] * w[1] - v[1] * w[0]], axis=0
    )
    cross = split_in_kernel(cross)
    loads[2].wait()
    part = split_dot((first[0], first[1]), cross)
    part = split_in_kernel(part)
    loads[3].wait()
    size = plan.rows * plan.groups
    total = None
    for i in range(2 * plan.slots):
        piece = tuple(p[i * size : (i + 1) * size] for p in part)
        term = split_dot(piece, (second[0, i], second[1, i]))
        total = term if total is None else total + term
    for s in range(plan.slabs):
        for r in range(plan.rows):
            send[s, :, r, :] = total[r * plan.groups : (r + 1) * plan.groups, s * 128 : (s + 1) * 128]

    pl.semaphore_wait(barrier, plan.count - 1)
    used = pl.ds(0, plan.rows)
    copies = []
    for i, offset in enumerate(offsets):
        to, source = spread(offset)
        copy = pltpu.make_async_remote_copy(
            src_ref=send.at[to[2], to[0] * plan.pens + to[1], used],
            dst_ref=recv.at[me, used],
            send_sem=send_sem.at[i],
            recv_sem=recv_sem.at[i],
            device_id=to,
            device_id_type=pl.DeviceIdType.MESH,
        )
        copy.start()
        arrival = pltpu.make_async_remote_copy(
            src_ref=send.at[to[2], to[0] * plan.pens + to[1], used],
            dst_ref=recv.at[source, used],
            send_sem=send_sem.at[i],
            recv_sem=recv_sem.at[i],
            device_id=to,
            device_id_type=pl.DeviceIdType.MESH,
        )
        copies.append((copy, arrival))
    recv[me, 0 : plan.rows] = send[slab, group, 0 : plan.rows]

    keep, bm, ky_n = plan.keep, plan.block, plan.rows_ky

    def signed(index):
        return jnp.where(index < keep // 2, index, index - keep)

    lane = lax.broadcasted_iota(jnp.int32, (keep, 128), 1)
    inner_lane = lax.rem(lane, plan.field)
    low_half = lane < plan.field
    is_real = lax.rem(lane // bm, 2) == 0
    kx = signed(lax.rem(lane, bm) + slab * bm)
    ky = signed(inner_lane // (2 * bm) + group * ky_n)
    kz = signed(lax.broadcasted_iota(jnp.int32, (keep, 128), 0))
    limit = -(keep // 2)
    mask = ((kx != limit) & (ky != limit) & (kz != limit)).astype(jnp.float32)
    kx, ky, kz = (k.astype(jnp.float32) for k in (kx, ky, kz))
    inverse = 1.0 / jnp.maximum(kx * kx + ky * ky + kz * kz, 1.0)
    pair = jnp.where(low_half, kx, ky)

    row = lax.broadcasted_iota(jnp.int32, (plan.field, keep), 0)
    kz_t = signed(lax.broadcasted_iota(jnp.int32, (plan.field, keep), 1)).astype(jnp.float32)
    kx_t = signed(lax.rem(row, bm) + slab * bm).astype(jnp.float32)
    ky_t = signed(row // (2 * bm) + group * ky_n).astype(jnp.float32)
    visc = 0.5 / (keep // 2) ** 2
    damp = visc * (kx_t * kx_t + ky_t * ky_t + kz_t * kz_t)
    loads[5].wait()
    damped = [damp * modes[c].reshape(plan.field, keep) for c in range(3)]
    loads[4].wait()

    for _, arrival in copies:
        arrival.wait_recv()
    got = split_in_kernel(recv[...].reshape(plan.count * 8, 128))
    out = split_dot((third[0], third[1]), got)
    out = [out[i * keep : (i + 1) * keep] for i in range(6)]

    def turn(cos_part, sin_part):
        ahead = pltpu.roll(sin_part, 128 - bm, 1)
        behind = pltpu.roll(sin_part, bm, 1)
        return cos_part + jnp.where(is_real, ahead, -behind)

    both = turn(out[0], out[1])
    last_cos = jnp.where(low_half, out[2], out[4])
    last_sin = jnp.where(low_half, out[3], out[5])
    last = turn(last_cos, last_sin)
    last = last + pltpu.roll(last, plan.field, 1)
    dots = pair * both
    inner = (dots + pltpu.roll(dots, plan.field, 1) + kz * last) * inverse
    both = jnp.transpose((both - pair * inner) * mask)
    last = jnp.transpose((last - kz * inner) * mask)
    shape = (ky_n, 2, bm, keep)
    out_ref[0] = (both[: plan.field] - damped[0]).reshape(shape)
    out_ref[1] = (both[plan.field :] - damped[1]).reshape(shape)
    out_ref[2] = (last[: plan.field] - damped[2]).reshape(shape)
    for copy, _ in copies:
        copy.wait_send()


def direct(plan, tables, velocity, vorticity, velocity_modes):
    modes = jnp.transpose(velocity_modes, (0, 2, 3, 4, 1))
    first, second, third = tables
    hbm = pl.BlockSpec(memory_space=pltpu.HBM)
    out = pl.pallas_call(
        functools.partial(kernel, plan),
        out_shape=pltpu.VMEM(modes.shape, jnp.float32),
        in_specs=[hbm] * 6,
        out_specs=pl.BlockSpec(memory_space=pltpu.VMEM),
        scratch_shapes=[
            pltpu.VMEM(velocity.shape, jnp.float32),
            pltpu.VMEM(vorticity.shape, jnp.float32),
            pltpu.VMEM(modes.shape, jnp.float32),
            pltpu.VMEM(first.shape[1:], jnp.bfloat16),
            pltpu.VMEM(second.shape, jnp.bfloat16),
            pltpu.VMEM(third.shape, jnp.bfloat16),
            pltpu.VMEM((plan.slabs, plan.groups, 8, 128), jnp.float32),
            pltpu.VMEM((plan.count, 8, 128), jnp.float32),
            pltpu.SemaphoreType.DMA((6,)),
            pltpu.SemaphoreType.DMA((plan.count - 1,)),
            pltpu.SemaphoreType.DMA((plan.count - 1,)),
        ],
        compiler_params=pltpu.CompilerParams(collective_id=0, has_side_effects=True),
    )(velocity, vorticity, modes, first, second, third)
    return jnp.transpose(out, (0, 4, 1, 2, 3))


def solution(mesh):
    sizes = dict(mesh.shape)

    def run(velocity, vorticity, velocity_modes):
        _, z_rows, y_rows, cells = velocity.shape
        plan = Plan(sizes, cells, velocity_modes.shape[1], z_rows, y_rows)
        if not plan.fits():
            return per_device(velocity, vorticity, velocity_modes)
        return direct(plan, plan.tables(), velocity, vorticity, velocity_modes)

    return jax.shard_map(
        run,
        mesh=mesh,
        in_specs=(
            P(None, ("section", "pen"), "slab", None),
            P(None, ("section", "pen"), "slab", None),
            P(None, None, ("section", "pen"), None, "slab"),
        ),
        out_specs=P(None, None, ("section", "pen"), None, "slab"),
        check_vma=False,
    )
```

```python
import functools
import math

import jax
import jax.numpy as jnp
import numpy as np
from jax import lax
from jax.experimental import pallas as pl
from jax.experimental.pallas import tpu as pltpu
from jax.sharding import PartitionSpec as P

AXES = ("section", "pen", "slab")
highest = lax.Precision.HIGHEST


def signed_modes(index, count):
    return jnp.where(index < count // 2, index, index - count)


def discrete_fourier_tables(length, keep_count):
    modes = signed_modes(jnp.arange(keep_count, dtype=jnp.int32), keep_count)
    mode_positions = jnp.arange(length, dtype=jnp.int32)
    phase = jnp.remainder(modes[:, None] * mode_positions[None, :], length).astype(jnp.float32)
    angles = 2.0 * math.pi / length * phase
    factor = 1.0 / math.sqrt(length)
    return (jnp.cos(angles) * factor, jnp.sin(angles) * factor)


def complex_apply(form, cosine, sine, real_part, imag_part):
    out_real = jnp.einsum(form, cosine, real_part, precision=highest) + jnp.einsum(
        form, sine, imag_part, precision=highest
    )
    out_imag = jnp.einsum(form, cosine, imag_part, precision=highest) - jnp.einsum(
        form, sine, real_part, precision=highest
    )
    return (out_real, out_imag)


def per_device(velocity, vorticity, velocity_modes):
    grid_cells = velocity.shape[3]
    keep_count = velocity_modes.shape[1]
    cross_product = jnp.stack(
        [
            velocity[1] * vorticity[2] - velocity[2] * vorticity[1],
            velocity[2] * vorticity[0] - velocity[0] * vorticity[2],
            velocity[0] * vorticity[1] - velocity[1] * vorticity[0],
        ]
    )
    slabs = lax.axis_size("slab")
    block_modes = keep_count // slabs
    cosine_table, sine_table = discrete_fourier_tables(grid_cells, keep_count)
    cols_real = cosine_table.T.reshape(grid_cells, slabs, block_modes)
    cols_imag = (-sine_table).T.reshape(grid_cells, slabs, block_modes)
    column_table = jnp.stack([cols_real, cols_imag], axis=2).reshape(grid_cells, 2 * keep_count)
    first_pass = jnp.einsum("czyx,xj->czyj", cross_product, column_table, precision=highest)
    block = lax.all_to_all(first_pass, "slab", split_axis=3, concat_axis=2, tiled=True)
    out_real, out_imag = complex_apply(
        "ky,czyj->czkj",
        cosine_table,
        sine_table,
        block[..., :block_modes],
        block[..., block_modes:],
    )
    second_pass = jnp.concatenate([out_real, out_imag], axis=-1)
    halves = lax.axis_size("section")
    pens = lax.axis_size("pen")
    rows_ky = keep_count // (halves * pens)
    block = lax.all_to_all(second_pass, ("section", "pen"), split_axis=2, concat_axis=1, tiled=True)
    out_real, out_imag = complex_apply(
        "kz,czyj->ckyj",
        cosine_table,
        sine_table,
        block[..., :block_modes],
        block[..., block_modes:],
    )
    third_pass = jnp.concatenate([out_real, out_imag], axis=-1)
    group_index = lax.axis_index("section") * pens + lax.axis_index("pen")
    modes_z = signed_modes(jnp.arange(keep_count, dtype=jnp.int32), keep_count)[:, None, None]
    modes_y = signed_modes(
        group_index * rows_ky + jnp.arange(rows_ky, dtype=jnp.int32), keep_count
    )[None, :, None]
    modes_x = signed_modes(
        lax.axis_index("slab") * block_modes + jnp.arange(block_modes, dtype=jnp.int32), keep_count
    )[None, None, :]
    limit = -(keep_count // 2)
    keep_mask = ((modes_x != limit) & (modes_y != limit) & (modes_z != limit)).astype(jnp.float32)
    waves = (modes_x.astype(jnp.float32), modes_y.astype(jnp.float32), modes_z.astype(jnp.float32))
    ksq = waves[0] * waves[0] + waves[1] * waves[1] + waves[2] * waves[2]
    denom = jnp.maximum(ksq, 1.0)
    parts = []
    for which in range(2):
        chosen = third_pass[..., which * block_modes : (which + 1) * block_modes]
        comp = [chosen[c] for c in range(3)]
        inner = (waves[0] * comp[0] + waves[1] * comp[1] + waves[2] * comp[2]) / denom
        parts.append(jnp.stack([comp[c] - waves[c] * inner for c in range(3)]))
    projected = jnp.stack(parts, axis=3)
    visc = 0.5 / (keep_count // 2) ** 2
    return (
        projected * keep_mask[None, :, :, None, :]
        - visc * ksq[None, :, :, None, :] * velocity_modes
    )


def split_bf16(table):
    high = table.astype(jnp.bfloat16)
    low = (table - high.astype(np.float32)).astype(jnp.bfloat16)
    return high, low


def split_in_kernel(value):
    high = value.astype(jnp.bfloat16)
    low = (value - high.astype(jnp.float32)).astype(jnp.bfloat16)
    return high, low


def mm(a, b):
    return lax.dot_general(a, b, (((1,), (0,)), ((), ())), preferred_element_type=jnp.float32)


def split_dot(a, b):
    return mm(a[0], b[0]) + mm(a[1], b[0]) + mm(a[0], b[1])


def wave_numbers(count):
    index = np.arange(count)
    return np.where(index < count // 2, index, index - count)


def host_tables(cells, keep):
    phase = np.remainder(wave_numbers(keep)[:, None] * np.arange(cells)[None, :], cells)
    angles = 2.0 * np.pi / cells * phase
    factor = 1.0 / np.sqrt(cells)
    return np.cos(angles) * factor, np.sin(angles) * factor


class Plan:
    def __init__(self, mesh_shape, cells, keep, z_rows, y_rows):
        self.cells, self.keep, self.z_rows, self.y_rows = cells, keep, z_rows, y_rows
        self.halves, self.pens, self.slabs = (mesh_shape[a] for a in AXES)
        self.groups = self.halves * self.pens
        self.count = self.groups * self.slabs
        self.rows_ky = keep // self.groups
        self.block = keep // self.slabs
        self.field = self.rows_ky * 2 * self.block
        self.rows = z_rows + (z_rows + 1) // 2
        self.slots = 2 * self.rows_ky

    def fits(self):
        return (
            2 * self.field == 128
            and self.rows <= 8
            and (self.rows * self.groups) % 16 == 0
            and self.y_rows % 8 == 0
            and self.keep % 8 == 0
            and self.block % 8 == 0
            and 3 * self.z_rows * self.y_rows <= 512
            and self.count <= 64
        )

    def place(self, comp, z):
        if comp < 2:
            return z, comp
        return self.z_rows + z // 2, z % 2

    def tables(self):
        cos, sin = host_tables(self.cells, self.keep)
        g, zl, yl, ky_n, bm = self.groups, self.z_rows, self.y_rows, self.rows_ky, self.block
        first = np.zeros((self.slabs, self.slots, 2, self.rows, g, 3, zl, yl), np.float32)
        for c in range(3):
            for z in range(zl):
                row, half = self.place(c, z)
                for ky in range(ky_n):
                    for s in range(self.slabs):
                        cells = slice(s * yl, (s + 1) * yl)
                        first[s, half * ky_n + ky, 0, row, :, c, z] = cos[ky::ky_n, cells]
                        first[s, half * ky_n + ky, 1, row, :, c, z] = -sin[ky::ky_n, cells]
        first = first.reshape(self.slabs, self.slots * 2 * self.rows * g, 3 * zl * yl)
        second = np.zeros((self.slots, 2, self.cells, self.slabs, self.slots, 2, bm), np.float32)
        for s in range(self.slabs):
            c_t = cos[s * bm : (s + 1) * bm].T
            s_t = sin[s * bm : (s + 1) * bm].T
            for q in range(self.slots):
                second[q, 0, :, s, q, 0] = c_t
                second[q, 0, :, s, q, 1] = -s_t
                second[q, 1, :, s, q, 0] = s_t
                second[q, 1, :, s, q, 1] = c_t
        second = second.reshape(self.slots, 2 * self.cells, self.slabs * 128)
        third = np.zeros((3, 2, self.keep, g, self.slabs, 8), np.float32)
        for z in range(zl):
            for which, table in enumerate((cos, sin)):
                column = table[:, z::zl][:, :, None]
                third[0, which, :, :, :, z] = column
                third[1 + z % 2, which, :, :, :, zl + z // 2] = column
        third = third.reshape(6 * self.keep, self.count * 8)
        return (
            np.stack(split_bf16(first), axis=1),
            np.stack(split_bf16(second)),
            np.stack(split_bf16(third)),
        )


def kernel(
    plan, vel_hbm, vort_hbm, modes_hbm, first_hbm, second_hbm, third_hbm, out_ref,
    vel, vort, modes, first, second, third, send, recv, load_sem, send_sem, recv_sem,
):
    sec, pen, slab = (lax.axis_index(a) for a in AXES)
    group = sec * plan.pens + pen
    me = group * plan.slabs + slab
    loads = [
        pltpu.make_async_copy(src, dst, load_sem.at[i])
        for i, (src, dst) in enumerate(
            (
                (vel_hbm, vel),
                (vort_hbm, vort),
                (first_hbm.at[slab], first),
                (second_hbm, second),
                (third_hbm, third),
                (modes_hbm, modes),
            )
        )
    ]
    for load in loads:
        load.start()

    def spread(offset):
        a, b, c = offset
        to = (
            lax.rem(sec + a, plan.halves),
            lax.rem(pen + b, plan.pens),
            lax.rem(slab + c, plan.slabs),
        )
        back = (
            lax.rem(sec + plan.halves - a, plan.halves),
            lax.rem(pen + plan.pens - b, plan.pens),
            lax.rem(slab + plan.slabs - c, plan.slabs),
        )
        return to, (back[0] * plan.pens + back[1]) * plan.slabs + back[2]

    offsets = [
        (a, b, c)
        for b in sorted(range(plan.pens), key=lambda v: -min(v, plan.pens - v))
        for a in reversed(range(plan.halves))
        for c in reversed(range(plan.slabs))
    ]
    offsets.remove((0, 0, 0))
    recv[...] = jnp.zeros_like(recv)
    barrier = pltpu.get_barrier_semaphore()
    for offset in offsets:
        pl.semaphore_signal(
            barrier, inc=1, device_id=spread(offset)[0], device_id_type=pl.DeviceIdType.MESH
        )

    loads[0].wait()
    loads[1].wait()
    zl, yl, cells = plan.z_rows, plan.y_rows, plan.cells
    v = [vel[c].reshape(zl * yl, cells) for c in range(3)]
    w = [vort[c].reshape(zl * yl, cells) for c in range(3)]
    cross = jnp.concatenate(
        [v[1] * w[2] - v[2] * w[1], v[2] * w[0] - v[0] * w[2], v[0] * w[1] - v[1] * w[0]], axis=0
    )
    cross = split_in_kernel(cross)
    loads[2].wait()
    part = split_dot((first[0], first[1]), cross)
    loads[3].wait()
    size = plan.rows * plan.groups
    total = None
    for i in range(plan.slots):
        halves = [part[j * size : (j + 1) * size] for j in (2 * i, 2 * i + 1)]
        piece = split_in_kernel(jnp.concatenate(halves, axis=1))
        term = split_dot(piece, (second[0, i], second[1, i]))
        total = term if total is None else total + term
    for s in range(plan.slabs):
        for r in range(plan.rows):
            send[s, :, r, :] = total[r * plan.groups : (r + 1) * plan.groups, s * 128 : (s + 1) * 128]

    pl.semaphore_wait(barrier, plan.count - 1)
    used = pl.ds(0, plan.rows)
    copies = []
    for i, offset in enumerate(offsets):
        to, source = spread(offset)
        copy = pltpu.make_async_remote_copy(
            src_ref=send.at[to[2], to[0] * plan.pens + to[1], used],
            dst_ref=recv.at[me, used],
            send_sem=send_sem.at[i],
            recv_sem=recv_sem.at[i],
            device_id=to,
            device_id_type=pl.DeviceIdType.MESH,
        )
        copy.start()
        arrival = pltpu.make_async_remote_copy(
            src_ref=send.at[to[2], to[0] * plan.pens + to[1], used],
            dst_ref=recv.at[source, used],
            send_sem=send_sem.at[i],
            recv_sem=recv_sem.at[i],
            device_id=to,
            device_id_type=pl.DeviceIdType.MESH,
        )
        copies.append((copy, arrival))
    recv[me, 0 : plan.rows] = send[slab, group, 0 : plan.rows]

    keep, bm, ky_n = plan.keep, plan.block, plan.rows_ky

    def signed(index):
        return jnp.where(index < keep // 2, index, index - keep)

    lane = lax.broadcasted_iota(jnp.int32, (keep, 128), 1)
    inner_lane = lax.rem(lane, plan.field)
    low_half = lane < plan.field
    is_real = lax.rem(lane // bm, 2) == 0
    kx = signed(lax.rem(lane, bm) + slab * bm)
    ky = signed(inner_lane // (2 * bm) + group * ky_n)
    kz = signed(lax.broadcasted_iota(jnp.int32, (keep, 128), 0))
    limit = -(keep // 2)
    mask = ((kx != limit) & (ky != limit) & (kz != limit)).astype(jnp.float32)
    kx, ky, kz = (k.astype(jnp.float32) for k in (kx, ky, kz))
    inverse = 1.0 / jnp.maximum(kx * kx + ky * ky + kz * kz, 1.0)
    pair = jnp.where(low_half, kx, ky)

    row = lax.broadcasted_iota(jnp.int32, (plan.field, keep), 0)
    kz_t = signed(lax.broadcasted_iota(jnp.int32, (plan.field, keep), 1)).astype(jnp.float32)
    kx_t = signed(lax.rem(row, bm) + slab * bm).astype(jnp.float32)
    ky_t = signed(row // (2 * bm) + group * ky_n).astype(jnp.float32)
    visc = 0.5 / (keep // 2) ** 2
    damp = visc * (kx_t * kx_t + ky_t * ky_t + kz_t * kz_t)
    loads[5].wait()
    damped = [damp * modes[c].reshape(plan.field, keep) for c in range(3)]
    loads[4].wait()

    for _, arrival in copies:
        arrival.wait_recv()
    got = split_in_kernel(recv[...].reshape(plan.count * 8, 128))
    out = split_dot((third[0], third[1]), got)
    out = [out[i * keep : (i + 1) * keep] for i in range(6)]

    def turn(cos_part, sin_part):
        ahead = pltpu.roll(sin_part, 128 - bm, 1)
        behind = pltpu.roll(sin_part, bm, 1)
        return cos_part + jnp.where(is_real, ahead, -behind)

    both = turn(out[0], out[1])
    last_cos = jnp.where(low_half, out[2], out[4])
    last_sin = jnp.where(low_half, out[3], out[5])
    last = turn(last_cos, last_sin)
    last = last + pltpu.roll(last, plan.field, 1)
    dots = pair * both
    inner = (dots + pltpu.roll(dots, plan.field, 1) + kz * last) * inverse
    both = jnp.transpose((both - pair * inner) * mask)
    last = jnp.transpose((last - kz * inner) * mask)
    shape = (ky_n, 2, bm, keep)
    out_ref[0] = (both[: plan.field] - damped[0]).reshape(shape)
    out_ref[1] = (both[plan.field :] - damped[1]).reshape(shape)
    out_ref[2] = (last[: plan.field] - damped[2]).reshape(shape)
    for copy, _ in copies:
        copy.wait_send()


def direct(plan, tables, velocity, vorticity, velocity_modes):
    modes = jnp.transpose(velocity_modes, (0, 2, 3, 4, 1))
    first, second, third = tables
    hbm = pl.BlockSpec(memory_space=pltpu.HBM)
    out = pl.pallas_call(
        functools.partial(kernel, plan),
        out_shape=pltpu.VMEM(modes.shape, jnp.float32),
        in_specs=[hbm] * 6,
        out_specs=pl.BlockSpec(memory_space=pltpu.VMEM),
        scratch_shapes=[
            pltpu.VMEM(velocity.shape, jnp.float32),
            pltpu.VMEM(vorticity.shape, jnp.float32),
            pltpu.VMEM(modes.shape, jnp.float32),
            pltpu.VMEM(first.shape[1:], jnp.bfloat16),
            pltpu.VMEM(second.shape, jnp.bfloat16),
            pltpu.VMEM(third.shape, jnp.bfloat16),
            pltpu.VMEM((plan.slabs, plan.groups, 8, 128), jnp.float32),
            pltpu.VMEM((plan.count, 8, 128), jnp.float32),
            pltpu.SemaphoreType.DMA((6,)),
            pltpu.SemaphoreType.DMA((plan.count - 1,)),
            pltpu.SemaphoreType.DMA((plan.count - 1,)),
        ],
        compiler_params=pltpu.CompilerParams(collective_id=0, has_side_effects=True),
    )(velocity, vorticity, modes, first, second, third)
    return jnp.transpose(out, (0, 4, 1, 2, 3))


def solution(mesh):
    sizes = dict(mesh.shape)

    def run(velocity, vorticity, velocity_modes):
        _, z_rows, y_rows, cells = velocity.shape
        plan = Plan(sizes, cells, velocity_modes.shape[1], z_rows, y_rows)
        if not plan.fits():
            return per_device(velocity, vorticity, velocity_modes)
        return direct(plan, plan.tables(), velocity, vorticity, velocity_modes)

    return jax.shard_map(
        run,
        mesh=mesh,
        in_specs=(
            P(None, ("section", "pen"), "slab", None),
            P(None, ("section", "pen"), "slab", None),
            P(None, None, ("section", "pen"), None, "slab"),
        ),
        out_specs=P(None, None, ("section", "pen"), None, "slab"),
        check_vma=False,
    )
```
